16 devices in a mesh: dp: 2 (over y, z), fsdp: 8 (over x, core).
Axes of the slice: x: 4, y: 2, z: 1, core: 2. Of those that a mesh axis runs over, the one named last changes fastest.
The devices are a block of a 4x4x8 slice.
Arguments:
- hidden: bfloat16 [2, 32768, 512], P(None, ('dp', 'fsdp')), parts along dimension 1
- targets: int32 [2, 32768], P(None, ('dp', 'fsdp')), parts along dimension 1
- w_out: bfloat16 [32128, 512], P('fsdp')
Outputs:
- output 1: float32 [4], P('dp'), parts along dimension 0
- output 2: float32 [2, 32768, 512], P(None, ('dp', 'fsdp')), parts along dimension 1
- output 3: float32 [64256, 512], P(('dp', 'fsdp')), parts along dimension 0
There are 2 independent parts. The reference program is written for one: setup_inputs(seed, part) draws one part's arguments, and reference() takes and returns one part's arrays. A program takes and returns all parts, laid end to end along the dimension named above; an argument that names none is the same for every part.
All inputs are finite; a program needn't handle non-finite values.
Results may differ from the reference program's by a relative error of at most 0.001.
Values are sent between devices in bfloat16 or wider.
A program may use at most 768 MiB of HBM per device.

```python
import jax
import jax.numpy as jnp
from jax import lax

TOK_DEV = 2048
GROUP_SIZE = 8
VOCAB_SIZE = 32128
MODEL_DIM = 512

TOKENS_PART = TOK_DEV * GROUP_SIZE
VOCAB_BLK = VOCAB_SIZE // GROUP_SIZE


def setup_inputs(seed: int = 0, part: int = 0) -> dict:
    base_key = jax.random.key(seed)
    shared_key, parts_key = jax.random.split(base_key)
    part_key = jax.random.fold_in(parts_key, part)
    key_hid, key_tgt = jax.random.split(part_key)
    hidden = jax.random.normal(key_hid, (2, TOKENS_PART, MODEL_DIM), jnp.float32).astype(jnp.bfloat16)
    targets = jax.random.randint(key_tgt, (2, TOKENS_PART), 0, VOCAB_SIZE, jnp.int32)
    targets = targets.at[0, 0].set(0).at[1, TOKENS_PART - 1].set(VOCAB_SIZE - 1)
    w_scaled = jax.random.normal(shared_key, (VOCAB_SIZE, MODEL_DIM), jnp.float32) * MODEL_DIM ** -0.5
    return {'hidden': hidden, 'targets': targets, 'w_out': w_scaled.astype(jnp.bfloat16)}


def reference(hidden, targets, w_out):
    tok_blocks = hidden.reshape(2 * GROUP_SIZE, TOK_DEV, MODEL_DIM)
    tgt_blocks = targets.reshape(2 * GROUP_SIZE, TOK_DEV)
    w_blocks = w_out.reshape(GROUP_SIZE, VOCAB_BLK, MODEL_DIM)
    blk_ids = jnp.arange(GROUP_SIZE, dtype=jnp.int32)
    col_ids = jnp.arange(VOCAB_BLK, dtype=jnp.int32)[None, :]

    def block_logits(tok_rows, row_tgt, w_blk, blk_idx):
        logits = jnp.dot(tok_rows, w_blk.T, preferred_element_type=jnp.float32)
        tgt_hit = (row_tgt - blk_idx * VOCAB_BLK)[:, None] == col_ids
        return logits, tgt_hit

    def token_stats(blk_in):
        tok_rows, row_tgt = blk_in

        def vocab_step(run_stats, w_in):
            run_max, run_sum, tgt_logit = run_stats
            logits, tgt_hit = block_logits(tok_rows, row_tgt, w_in[0], w_in[1])
            tgt_logit = tgt_logit + jnp.sum(jnp.where(tgt_hit, logits, 0.0), axis=1)
            new_max = jnp.maximum(run_max, jnp.max(logits, axis=1))
            run_sum = run_sum * jnp.exp(run_max - new_max) + jnp.sum(jnp.exp(logits - new_max[:, None]), axis=1)
            return (new_max, run_sum, tgt_logit), None

        init_stats = (jnp.full((TOK_DEV,), -jnp.inf, jnp.float32), jnp.zeros((TOK_DEV,), jnp.float32), jnp.zeros((TOK_DEV,), jnp.float32))
        (run_max, run_sum, tgt_logit), _ = lax.scan(vocab_step, init_stats, (w_blocks, blk_ids))
        return run_max + jnp.log(run_sum), tgt_logit

    log_norm, tgt_logit = lax.map(token_stats, (tok_blocks, tgt_blocks))
    loss_vals = jnp.sum((log_norm - tgt_logit).reshape(2, TOKENS_PART), axis=1) / TOKENS_PART

    def token_grads(d_w, blk_in):
        tok_rows, row_tgt, row_norm = blk_in

        def vocab_step(d_rows, w_in):
            logits, tgt_hit = block_logits(tok_rows, row_tgt, w_in[0], w_in[1])
            soft_probs = jnp.exp(logits - row_norm[:, None])
            d_logits = ((soft_probs - tgt_hit.astype(jnp.float32)) / TOKENS_PART).astype(jnp.bfloat16)
            d_rows = d_rows + jnp.dot(d_logits, w_in[0], preferred_element_type=jnp.float32)
            d_w_blk = jnp.dot(d_logits.T, tok_rows, preferred_element_type=jnp.float32)
            return d_rows, d_w_blk

        d_rows, d_w_blocks = lax.scan(vocab_step, jnp.zeros((TOK_DEV, MODEL_DIM), jnp.float32), (w_blocks, blk_ids))
        return d_w + d_w_blocks.reshape(VOCAB_SIZE, MODEL_DIM), d_rows

    d_w, d_rows = lax.scan(token_grads, jnp.zeros((VOCAB_SIZE, MODEL_DIM), jnp.float32), (tok_blocks, tgt_blocks, log_norm))
    return loss_vals, d_rows.reshape(2, TOKENS_PART, MODEL_DIM), d_w
```

```python
import functools

import jax
import jax.numpy as jnp
from jax import lax
from jax.experimental import pallas as pl
from jax.experimental.pallas import tpu as pltpu
from jax.sharding import PartitionSpec as P

F32, BF16, I32 = jnp.float32, jnp.bfloat16, jnp.int32
LOG2E = 1.4426950408889634
LN2 = 0.6931471805599453
BT = 1024
RC = 256
VMEM_LIMIT = 60 << 20
ANY = pl.BlockSpec(memory_space=pl.ANY)
VM = pl.BlockSpec(memory_space=pltpu.VMEM)


def chunks(rows):
    return [(r0, min(RC, rows - r0)) for r0 in range(0, rows, RC)]


def up(a, b):
    return -(-a // b) * b


def fwd_unit(w_ref, h_ref, z_ref, m_ref, s_ref, t_ref, tgt):
    rows = w_ref.shape[0]
    h = h_ref[...]
    tj = tgt - lax.broadcasted_iota(I32, (8, BT), 0)
    m, s, t = m_ref[...], s_ref[...], t_ref[...]
    for r0, rc in chunks(rows):
        z = lax.dot_general(w_ref[r0:r0 + rc, :], h, (((1,), (1,)), ((), ())), preferred_element_type=F32) * LOG2E
        z_ref[r0:r0 + rc, :] = z
        z = z.reshape(rc // 8, 8, BT)
        mn = jnp.maximum(m, jnp.max(z, axis=0))
        s = s * jnp.exp2(m - mn) + jnp.sum(jnp.exp2(z - mn[None]), axis=0)
        m = mn
        for k in range(rc // 8):
            t = jnp.where(tj == r0 + 8 * k, z[k], t)
    m_ref[...], s_ref[...], t_ref[...] = m, s, t


def bwd_unit(z_ref, lse, tgt, inv, wt_ref, h_ref, dw_ref, dh_ref):
    rows = z_ref.shape[0]
    h = h_ref[...]
    tj = tgt - lax.broadcasted_iota(I32, (8, BT), 0)
    acc = None
    for r0, rc in chunks(rows):
        z = z_ref[r0:r0 + rc, :].reshape(rc // 8, 8, BT)
        p = jnp.exp2(z - lse[None])
        row = lax.broadcasted_iota(I32, (rc // 8, 8, BT), 0) * 8 + r0
        dz = jnp.where(row == tj[None], p - inv, p).reshape(rc, BT)
        rk, rm = up(rc, 256), up(rc, 16)
        if rk > rc:
            dz = jnp.concatenate([dz, jnp.zeros((rk - rc, BT), F32)], axis=0)
        dz = dz.astype(BF16)
        d = jnp.dot(dz[:rm], h, preferred_element_type=F32)
        dw_ref[r0:r0 + rc, :] += d[:rc]
        d = jnp.dot(wt_ref[:, r0:r0 + rk], dz, preferred_element_type=F32)
        acc = d if acc is None else acc + d
    dh_ref[...] += acc


def fwd_kernel(n_half, n_blk, w0, w1, hbuf, tgt, base, z, st, wv, hv, zv, m, s, t, w_sem, h_sem, z_sem):
    rows = wv.shape[1]
    n_units = n_half * n_blk
    for k in range(n_half):
        src = (w0, w1)[k // 2]
        pltpu.make_async_copy(src.at[pl.ds((k % 2) * rows, rows)], wv.at[k], w_sem.at[k]).start()

    def load_h(u, slot):
        return pltpu.make_async_copy(hbuf.at[lax.rem(u, n_blk)], hv.at[slot], h_sem.at[slot])

    def store_z(u, slot):
        return pltpu.make_async_copy(zv.at[slot], z.at[u // n_blk, lax.rem(u, n_blk)], z_sem.at[slot])

    load_h(0, 0).start()
    m[...] = jnp.full_like(m, -jnp.inf)
    s[...] = jnp.zeros_like(s)
    t[...] = jnp.zeros_like(t)

    @pl.loop(0, n_units)
    def _(u):
        slot = lax.rem(u, 2)
        half, blk = u // n_blk, lax.rem(u, n_blk)

        @pl.when(blk == 0)
        def _():
            pltpu.make_async_copy(w0.at[pl.ds(0, rows)], wv.at[half], w_sem.at[half]).wait()

        load_h(u, slot).wait()

        @pl.when(u + 1 < n_units)
        def _():
            load_h(u + 1, 1 - slot).start()

        @pl.when(u >= 2)
        def _():
            store_z(u - 2, slot).wait()

        fwd_unit(wv.at[half], hv.at[slot], zv.at[slot], m.at[blk], s.at[blk], t.at[blk], tgt[blk] - base[half])
        store_z(u, slot).start()

    m1 = jnp.max(m[...], axis=1, keepdims=True)
    st[0] = m1[:, 0, :]
    st[1] = jnp.sum(s[...] * jnp.exp2(m[...] - m1), axis=1)
    st[2] = jnp.sum(t[...], axis=1)
    store_z(n_units - 2, 0).wait()
    store_z(n_units - 1, 1).wait()


def bwd_kernel(n_half, n_blk, inv, w0, w1, hbuf, tgt, base, lse, z, dw, dh, wv, wt, hv, zv, dwa, dha, w_sem, h_sem, z_sem, o_sem):
    rows = zv.shape[1]
    cols = wt.shape[2]
    n_units = n_half * n_blk

    def load_w(k):
        src = (w0, w1)[k // 2]
        return pltpu.make_async_copy(src.at[pl.ds((k % 2) * rows, rows)], wv, w_sem)

    def load_h(u, slot):
        return pltpu.make_async_copy(hbuf.at[u // n_half], hv.at[slot], h_sem.at[slot])

    def load_z(u, slot):
        return pltpu.make_async_copy(z.at[lax.rem(u, n_half), u // n_half], zv.at[slot], z_sem.at[slot])

    load_z(0, 0).start()
    load_h(0, 0).start()
    for k in range(n_half):
        load_w(k).start()
        load_w(k).wait()
        for r0, rc in chunks(rows):
            wt[k, :, r0:r0 + rc] = wv[r0:r0 + rc, :].T
        if cols > rows:
            wt[k, :, rows:] = jnp.zeros((wt.shape[1], cols - rows), BF16)
    dwa[...] = jnp.zeros_like(dwa)

    @pl.loop(0, n_units)
    def _(u):
        slot = lax.rem(u, 2)
        half, blk = lax.rem(u, n_half), u // n_half
        hslot = lax.rem(blk, 2)
        load_z(u, slot).wait()

        @pl.when(u + 1 < n_units)
        def _():
            load_z(u + 1, 1 - slot).start()

        @pl.when(half == 0)
        def _():
            pltpu.make_async_copy(hbuf.at[blk], hv.at[hslot], h_sem.at[hslot]).wait()

            @pl.when(blk + 1 < n_blk)
            def _():
                pltpu.make_async_copy(hbuf.at[blk + 1], hv.at[1 - hslot], h_sem.at[1 - hslot]).start()

            @pl.when(blk >= 2)
            def _():
                pltpu.make_async_copy(dha.at[hslot], dh.at[blk], o_sem.at[hslot]).wait()

            dha[hslot] = jnp.zeros(dha.shape[1:], F32)

        bwd_unit(zv.at[slot], lse[blk], tgt[blk] - base[half], inv, wt.at[half], hv.at[hslot], dwa.at[half], dha.at[hslot])

        @pl.when(half == n_half - 1)
        def _():
            pltpu.make_async_copy(dha.at[hslot], dh.at[blk], o_sem.at[hslot]).start()

    for k in range(2):
        pltpu.make_async_copy(dha.at[k], dh.at[0], o_sem.at[k]).wait()
    pltpu.make_async_copy(dwa, dw, w_sem).start()
    pltpu.make_async_copy(dwa, dw, w_sem).wait()


def solution(mesh):
    group_size = mesh.shape['fsdp']
    n_chips = group_size // 2
    quads = [list(range(q, q + 4)) for q in range(0, group_size, 4)]

    def vocab_peer(f):
        chip, core = f // 2, f % 2
        other = (chip + 1) % n_chips if chip % 2 else (chip - 1) % n_chips
        return other * 2 + core

    peer_perm = [(f, vocab_peer(f)) for f in range(group_size)]

    def local_head(hidden, targets, w_loc):
        n_micro, tok_dev, dim = hidden.shape
        vb = w_loc.shape[0]
        tokens = tok_dev * group_size
        rows = vb // 2
        n_own = n_micro * tok_dev // BT
        n_blk, n_half = 4 * n_own, 4
        me = lax.axis_index('fsdp')
        chip, core = me // 2, lax.rem(me, 2)
        step = 2 * lax.rem(chip, 2) - 1
        peer = lax.rem(chip + step + n_chips, n_chips) * 2 + core
        base = jnp.stack([me * vb, me * vb + rows, peer * vb, peer * vb + rows]).astype(I32)

        hbuf = lax.all_gather(hidden.reshape(n_own, BT, dim), 'fsdp', axis_index_groups=quads, tiled=True)
        tgt = lax.all_gather(targets.reshape(n_own, 1, BT), 'fsdp', axis_index_groups=quads, tiled=True)
        w_peer = lax.ppermute(w_loc, 'fsdp', peer_perm)

        z, st = pl.pallas_call(
            functools.partial(fwd_kernel, n_half, n_blk),
            out_shape=(jax.ShapeDtypeStruct((n_half, n_blk, rows, BT), F32), jax.ShapeDtypeStruct((3, n_blk, BT), F32)),
            in_specs=[ANY, ANY, ANY, VM, pl.BlockSpec(memory_space=pltpu.SMEM)],
            out_specs=(ANY, VM),
            scratch_shapes=[
                pltpu.VMEM((n_half, rows, dim), BF16), pltpu.VMEM((2, BT, dim), BF16), pltpu.VMEM((2, rows, BT), F32),
                pltpu.VMEM((n_blk, 8, BT), F32), pltpu.VMEM((n_blk, 8, BT), F32), pltpu.VMEM((n_blk, 8, BT), F32),
                pltpu.SemaphoreType.DMA((n_half,)), pltpu.SemaphoreType.DMA((2,)), pltpu.SemaphoreType.DMA((2,))],
            compiler_params=pltpu.CompilerParams(vmem_limit_bytes=VMEM_LIMIT), name='fwd',
        )(w_loc, w_peer, hbuf, tgt, base)

        sts = lax.all_gather(st, 'fsdp', axis_index_groups=quads)
        mx = jnp.max(sts[:, 0], axis=0)
        lse2 = mx + jnp.log2(jnp.sum(sts[:, 1] * jnp.exp2(sts[:, 0] - mx[None]), axis=0))
        tl = jnp.sum(sts[:, 2], axis=0)
        tok_loss = ((lse2 - tl) * LN2).reshape(4, n_micro, tok_dev)
        mine = lax.dynamic_index_in_dim(tok_loss, lax.rem(me, 4), 0, keepdims=False)
        loss = lax.psum(jnp.sum(mine, axis=1) / tokens, 'fsdp')
        lse_t = (lse2 + jnp.log2(jnp.float32(tokens))).reshape(n_blk, 1, BT)

        dw, dh = pl.pallas_call(
            functools.partial(bwd_kernel, n_half, n_blk, 1.0 / tokens),
            out_shape=(jax.ShapeDtypeStruct((n_half, rows, dim), F32), jax.ShapeDtypeStruct((n_blk, dim, BT), F32)),
            in_specs=[ANY, ANY, ANY, VM, pl.BlockSpec(memory_space=pltpu.SMEM), VM, ANY],
            out_specs=(ANY, ANY),
            scratch_shapes=[
                pltpu.VMEM((rows, dim), BF16), pltpu.VMEM((n_half, dim, up(rows, 256)), BF16), pltpu.VMEM((2, BT, dim), BF16),
                pltpu.VMEM((2, rows, BT), F32), pltpu.VMEM((n_half, rows, dim), F32), pltpu.VMEM((2, dim, BT), F32),
                pltpu.SemaphoreType.DMA, pltpu.SemaphoreType.DMA((2,)), pltpu.SemaphoreType.DMA((2,)), pltpu.SemaphoreType.DMA((2,))],
            compiler_params=pltpu.CompilerParams(vmem_limit_bytes=VMEM_LIMIT), name='bwd',
        )(w_loc, w_peer, hbuf, tgt, base, lse_t, z)

        dw = dw.reshape(2, vb, dim)
        d_w = dw[0] + lax.ppermute(dw[1], 'fsdp', peer_perm)
        d_h = lax.psum_scatter(dh, 'fsdp', axis_index_groups=quads, tiled=True)
        d_h = d_h.transpose(0, 2, 1).reshape(n_micro, tok_dev, dim)
        return loss, d_h, d_w

    return jax.shard_map(local_head, mesh=mesh,
                         in_specs=(P(None, ('dp', 'fsdp'), None), P(None, ('dp', 'fsdp')), P('fsdp', None)),
                         out_specs=(P('dp'), P(None, ('dp', 'fsdp'), None), P(('dp', 'fsdp'), None)),
                         check_vma=False)
```

```python
import functools
import math

import jax
import jax.numpy as jnp
from jax import lax
from jax.experimental import pallas as pl
from jax.experimental.pallas import tpu as pltpu
from jax.sharding import PartitionSpec as P

F32, BF16, I32 = jnp.float32, jnp.bfloat16, jnp.int32
LOG2E = 1.4426950408889634
LN2 = 0.6931471805599453
BT = 1024
RC = 256
VMEM_LIMIT = 61 << 20
ANY = pl.BlockSpec(memory_space=pl.ANY)
VM = pl.BlockSpec(memory_space=pltpu.VMEM)
DMA = pltpu.SemaphoreType.DMA
local = pltpu.make_async_copy


def remote(src, dst, send_sem, recv_sem, to):
    return pltpu.make_async_remote_copy(src_ref=src, dst_ref=dst, send_sem=send_sem, recv_sem=recv_sem,
                                        device_id={'fsdp': to}, device_id_type=pl.DeviceIdType.MESH)


def chunks(rows):
    return [(r0, min(RC, rows - r0)) for r0 in range(0, rows, RC)]


def up(a, b):
    return -(-a // b) * b


def pick(x, segments):
    out = segments[0][1]
    for lo, vals in segments[1:]:
        out = tuple(jnp.where(x >= lo, a, b) for a, b in zip(vals, out))
    return out


class Place:
    def __init__(self, n):
        self.me = lax.axis_index('fsdp')
        self.chip, self.core = self.me // 2, lax.rem(self.me, 2)
        self.odd = lax.rem(self.chip, 2)
        self.sib = self.me + 1 - 2 * self.core
        self.par = self.me + 2 - 4 * self.odd
        self.diag = self.sib + 2 - 4 * self.odd
        self.peer = lax.rem(self.chip + 2 * self.odd - 1 + n // 2, n // 2) * 2 + self.core

    def share(self, r):
        a, b = lax.rem(r, 2), r // 2
        return 2 * (self.odd + b - 2 * self.odd * b) + self.core + a - 2 * self.core * a


def barrier_with(others):
    sem = pltpu.get_barrier_semaphore()
    for d in others:
        pl.semaphore_signal(sem, inc=1, device_id={'fsdp': d}, device_id_type=pl.DeviceIdType.MESH)
    pl.semaphore_wait(sem, len(others))


def fwd_unit(w_ref, h_ref, z_ref, m_ref, s_ref):
    rows = w_ref.shape[0]
    h = h_ref[...]
    m, s = m_ref[...], s_ref[...]
    for r0, rc in chunks(rows):
        z = lax.dot_general(w_ref[r0:r0 + rc, :], h, (((1,), (1,)), ((), ())), preferred_element_type=F32) * LOG2E
        z_ref[r0:r0 + rc, :] = z
        z = z.reshape(rc // 8, 8, BT)
        mn = jnp.maximum(m, jnp.max(z, axis=0))
        s = s * jnp.exp2(m - mn) + jnp.sum(jnp.exp2(z - mn[None]), axis=0)
        m = mn
    m_ref[...], s_ref[...] = m, s


def bwd_unit(z_ref, lse, tgt, inv, wt_ref, h_ref, dw_ref, dh_ref, tl_ref):
    rows = z_ref.shape[0]
    h = h_ref[...]
    tj = tgt - lax.broadcasted_iota(I32, (8, BT), 0)
    tl = jnp.zeros((8, BT), F32)
    acc = None
    for r0, rc in chunks(rows):
        z = z_ref[r0:r0 + rc, :].reshape(rc // 8, 8, BT)
        p = jnp.exp2(z - lse[None])
        hit = lax.broadcasted_iota(I32, (rc // 8, 8, BT), 0) * 8 + r0 == tj[None]
        dz = jnp.where(hit, p - inv, p).reshape(rc, BT)
        for k in range(rc // 8):
            tl = jnp.where(hit[k], z[k], tl)
        rk, rm = up(rc, 256), up(rc, 16)
        if rk > rc:
            dz = jnp.concatenate([dz, jnp.zeros((rk - rc, BT), F32)], axis=0)
        dz = dz.astype(BF16)
        d = jnp.dot(dz[:rm], h, preferred_element_type=F32)
        dw_ref[r0:r0 + rc, :] += d[:rc]
        d = jnp.dot(wt_ref[:, r0:r0 + rk], dz, preferred_element_type=F32)
        acc = d if acc is None else acc + d
    dh_ref[...] += acc
    tl_ref[...] += tl


def fwd_kernel(n, tokens, hid, w, tg, z, lse, hbuf, wpeer, tall, wv, hv, zv, m, s, st, strx,
               rh, lw, rw, sw, shs, shp, sf, stt, rt, lt, oh, ow, oz, ss, rs):
    at = Place(n)
    n_own = hid.shape[0]
    rows = wv.shape[1]
    quad = (at.me, at.sib, at.par, at.diag)

    def blk(r, b):
        return n_own * at.share(r) + b

    half_src = [w.at[pl.ds(k * rows, rows)] for k in range(2)]
    for k in range(2):
        local(half_src[k], wv.at[k], lw.at[k]).start()
    for b in range(n_own):
        local(hid.at[b], hv.at[blk(0, b)], rh.at[b]).start()
    own_t = tall.at[pl.ds(n_own * at.share(0), n_own)]
    local(tg, own_t, lt).start()

    barrier_with([at.sib, at.par, at.diag, at.peer])

    def send_sib(b):
        return remote(hid.at[b], hv.at[blk(0, b)], shs.at[b], rh.at[n_own + b], at.sib)

    def send_par(b):
        return remote(hid.at[b], hv.at[blk(0, b)], shp.at[b], rh.at[2 * n_own + b], at.par)

    def forward(b):
        return remote(hv.at[blk(2, b)], hv.at[blk(2, b)], sf.at[b], rh.at[3 * n_own + b], at.sib)

    def send_w(k):
        return remote(half_src[k], wv.at[2 + k], sw.at[k], rw.at[k], at.peer)

    def send_t(r):
        return remote(tg, own_t, stt.at[r - 1], rt.at[r - 1], quad[r])

    def send_st(r):
        return remote(st, strx.at[r - 1], ss.at[r - 1], rs.at[r - 1], quad[r])

    for k in range(n_own):
        send_sib(k).start()
        send_par(k).start()
        if k < 2:
            send_w(k).start()
    for r in range(1, 4):
        send_t(r).start()

    m[...] = jnp.full_like(m, -jnp.inf)
    s[...] = jnp.zeros_like(s)

    n1 = 4 * n_own
    def order(u):
        def near(q):
            return lax.rem(q, 2), q // (2 * n_own), lax.rem(q // 2, n_own)

        def far(q, b0):
            return lax.rem(q, 2), 2 + lax.rem(q // 2, 2), b0 + q // 4

        def wide(q, h):
            return jnp.full_like(q, h), q // n_own, lax.rem(q, n_own)

        s2, s3 = n1, n1 + 4
        s4 = s3 + 2 * n_own
        s5 = s4 + 4 * (n_own - 2)
        s6 = s5 + 2 * n_own
        s7 = s6 + 4
        h7, r7, b7 = far(u - s7, 0)
        return pick(u, [(0, near(u)), (s2, far(u - s2, 0)), (s3, wide(u - s3, 2)), (s4, far(u - s4, 1)),
                        (s5, wide(u - s5, 3)), (s6, far(u - s6, n_own - 1)), (s7, (h7 + 2, r7, b7))]), s3, s5

    n_units = 4 * 4 * n_own

    def store_z(u):
        (h, r, b), _, _ = order(u)
        slot = lax.rem(u, 3)
        return local(zv.at[slot], z.at[h, blk(r, b)], oz.at[slot])

    def wait_z(slot):
        local(zv.at[slot], z.at[0, 0], oz.at[slot]).wait()

    @pl.loop(0, n_units)
    def _(u):
        slot = lax.rem(u, 3)
        (h, r, b), first2, first3 = order(u)
        i = blk(r, b)

        @pl.when(u < 2)
        def _():
            local(half_src[0], wv.at[u], lw.at[u]).wait()

        @pl.when(jnp.logical_or(u == first2, u == first3))
        def _():
            remote(half_src[0], wv.at[h], sw.at[0], rw.at[h - 2], at.peer).wait_recv()
            local(wv.at[h], wpeer.at[h - 2], ow.at[h - 2]).start()

        @pl.when(h == 0)
        def _():
            @pl.when(r == 0)
            def _():
                local(hid.at[0], hv.at[i], rh.at[b]).wait()

            @pl.when(r > 0)
            def _():
                remote(hid.at[0], hv.at[i], shs.at[0], rh.at[n_own * r + b], at.sib).wait_recv()

            local(hv.at[i], hbuf.at[i], oh.at[i]).start()

            @pl.when(r == 2)
            def _():
                forward(b).start()

        @pl.when(u >= 3)
        def _():
            wait_z(slot)

        fwd_unit(wv.at[h], hv.at[i], zv.at[slot], m.at[i], s.at[i])
        store_z(u).start()

    mm = m[...]
    m1 = jnp.max(mm, axis=1, keepdims=True)
    st[0] = m1[:, 0, :]
    st[1] = jnp.sum(s[...] * jnp.exp2(mm - m1), axis=1)
    for r in range(1, 4):
        send_st(r).start()
    for r in range(1, 4):
        send_t(r).wait()
        send_st(r).wait()
    mx = st[0]
    for r in range(3):
        mx = jnp.maximum(mx, strx[r, 0])
    tot = st[1] * jnp.exp2(st[0] - mx)
    for r in range(3):
        tot = tot + strx[r, 1] * jnp.exp2(strx[r, 0] - mx)
    lse[...] = (mx + jnp.log(tot) * LOG2E + math.log2(tokens)).reshape(lse.shape)

    local(tg, own_t, lt).wait()
    for k in range(n_own):
        send_sib(k).wait_send()
        send_par(k).wait_send()
        forward(k).wait_send()
    for k in range(2):
        send_w(k).wait_send()
        local(wv.at[2 + k], wpeer.at[k], ow.at[k]).wait()
    for k in range(4 * n_own):
        local(hv.at[k], hbuf.at[k], oh.at[k]).wait()
    for k in range(3):
        wait_z(k)


def bwd_kernel(n, tokens, n_micro, w, wpeer, hbuf, tall, lse, z, dwo, rxw, dho, loss, part, rxs, txb, rxb, zblk,
               wv, wt, hv, zv, dwa, dha, rbuf, tla, lmsg, lrx,
               lw, lz, lh, li, lr, eo, es, rss, sb, rb, swr, rwr, sl, rl):
    at = Place(n)
    n_own = dho.shape[0]
    rows, cols = zv.shape[1], wt.shape[2]
    inv = 1.0 / tokens

    sem = pltpu.get_barrier_semaphore()
    for d in range(1, n):
        pl.semaphore_signal(sem, inc=1, device_id={'fsdp': lax.rem(at.me + d, n)}, device_id_type=pl.DeviceIdType.MESH)

    def blk(r, b):
        return n_own * at.share(r) + b

    far = 2 * (n_own - 1)
    v_b, v_c = 2, 2 + far + 2 * n_own
    v_d = v_c + far - 2
    v_e = v_d + 2 + 2 * n_own
    v_f = v_e + 2
    n_visits = v_f + 2 * n_own
    u_b = 8
    u_c = u_b + far + 2 * n_own
    u_d = u_c + 3 * (far - 2)
    u_e = u_d + 2 + 2 * n_own
    u_f = u_e + 4
    n_units = u_f + 4 * n_own

    def visit(v):
        def far_pair(q, b0):
            return 3 - lax.rem(q, 2), b0 + q // 2

        def near_pair(q):
            return 1 - lax.rem(q, 2), q // 2

        one = jnp.ones_like(v)
        zero = one - 1
        qb, qc, qd, qe, qf = v - v_b, v - v_c, v - v_d, v - v_e, v - v_f
        return pick(v, [
            (0, (4 * one, *far_pair(v, 0), zero, 4 * v, one, one)),
            (v_b, (one, *far_pair(qb, 1), 2 * one, u_b + qb, one, zero)),
            (v_b + far, (one, *near_pair(qb - far), 2 * one, u_b + qb, one, zero)),
            (v_c, (3 * one, *far_pair(qc, 1), 3 * one, u_c + 3 * qc, zero, one)),
            (v_d, (one, *far_pair(qd, n_own - 1), 3 * one, u_d + qd, zero, zero)),
            (v_d + 2, (one, *near_pair(qd - 2), 3 * one, u_d + qd, zero, zero)),
            (v_e, (2 * one, *far_pair(qe, n_own - 1), zero, u_e + 2 * qe, zero, one)),
            (v_f, (2 * one, *near_pair(qf), zero, u_f + 2 * qf, zero, one)),
        ])

    def load_z(h, i, slot):
        return local(z.at[h, i], zv.at[slot], lz.at[slot])

    def load_h(i, slot):
        return local(hbuf.at[i], hv.at[slot], lh.at[slot])

    def start_init(i, fresh, slot):
        @pl.when(fresh == 1)
        def _():
            local(zblk, dha.at[slot], li.at[slot]).start()

        @pl.when(fresh == 0)
        def _():
            local(part.at[i], dha.at[slot], li.at[slot]).start()

    def to_sib(r, b, slot):
        return remote(dha.at[slot], rxs.at[n_own * (1 - r // 2) + b], es.at[slot], rss.at[n_own * (1 - r // 2) + b], at.sib)

    def from_sib(r, b):
        return remote(dha.at[0], rxs.at[n_own * (1 - r // 2) + b], es.at[0], rss.at[n_own * (1 - r // 2) + b], at.sib)

    def to_par(b):
        return remote(txb.at[b], rxb.at[b], sb.at[b], rb.at[b], at.par)

    def to_peer(k):
        return remote(dwa.at[2 + k], rxw.at[k], swr.at[k], rwr.at[k], at.peer)

    load_z(0, blk(3, 0), 0).start()
    load_h(blk(3, 0), 0).start()
    rbuf[0] = jnp.zeros(rbuf.shape[1:], F32)
    local(rbuf.at[0], zblk, lr.at[0]).start()
    halves = [w.at[pl.ds(0, rows)], w.at[pl.ds(rows, rows)], wpeer.at[0], wpeer.at[1]]
    local(halves[0], wv.at[0], lw.at[0]).start()
    dwa[...] = jnp.zeros_like(dwa)
    tla[...] = jnp.zeros_like(tla)
    for k in range(4):
        local(halves[k], wv.at[k % 2], lw.at[k % 2]).wait()
        if k < 3:
            local(halves[k + 1], wv.at[(k + 1) % 2], lw.at[(k + 1) % 2]).start()
        for r0, rc in chunks(rows):
            wt[k, :, r0:r0 + rc] = wv[k % 2, r0:r0 + rc, :].T
        if cols > rows:
            wt[k, :, rows:] = jnp.zeros((wt.shape[1], cols - rows), BF16)
    local(rbuf.at[0], zblk, lr.at[0]).wait()
    local(zblk, dha.at[0], li.at[0]).start()
    pl.semaphore_wait(sem, n - 1)

    def finish(v):
        slot = lax.rem(v, 3)
        _, r, b, _, _, _, comp = visit(v)
        sent = jnp.logical_and(comp == 1, lax.rem(r, 2) == 1)

        @pl.when(sent)
        def _():
            to_sib(r, b, slot).wait_send()

        @pl.when(jnp.logical_not(sent))
        def _():
            local(dha.at[slot], part.at[0], eo.at[slot]).wait()

        @pl.when(jnp.logical_and(comp == 1, r == 2))
        def _():
            to_par(b).start()

    @pl.loop(0, n_visits)
    def _(v):
        count, r, b, h0, u0, _, comp = visit(v)
        _, r_n, b_n, h0_n, _, fresh_n, _ = visit(v + 1)
        i, i_n = blk(r, b), blk(r_n, b_n)
        hs, ds = lax.rem(v, 2), lax.rem(v, 3)
        mine = jnp.logical_and(comp == 1, lax.rem(r, 2) == 0)
        last = jnp.logical_and(mine, r == 0)

        @pl.when(v >= 2)
        def _():
            finish(v - 2)

        local(zblk, dha.at[ds], li.at[ds]).wait()
        load_h(i, hs).wait()

        @pl.when(v + 1 < n_visits)
        def _():
            start_init(i_n, fresh_n, lax.rem(v + 1, 3))
            load_h(i_n, 1 - hs).start()

        @pl.loop(0, count)
        def _(k):
            u = u0 + k
            slot = lax.rem(u, 2)
            h = lax.rem(h0 + k, 4)
            end = k + 1 == count
            load_z(h, i, slot).wait()

            @pl.when(u + 1 < n_units)
            def _():
                load_z(jnp.where(end, h0_n, lax.rem(h + 1, 4)), jnp.where(end, i_n, i), 1 - slot).start()

            @pl.when(jnp.logical_and(end, mine))
            def _():
                from_sib(r, b).wait_recv()
                local(rxs.at[n_own * (1 - r // 2) + b], rbuf.at[0], lr.at[0]).start()

            @pl.when(jnp.logical_and(end, last))
            def _():
                to_par(b).wait_recv()
                local(rxb.at[b], rbuf.at[1], lr.at[1]).start()

            base = jnp.where(h < 2, at.me, at.peer) * (2 * rows) + lax.rem(h, 2) * rows
            bwd_unit(zv.at[slot], lse[i], tall[i] - base, inv, wt.at[h], hv.at[hs], dwa.at[h], dha.at[ds],
                     tla.at[b // (n_own // n_micro)])

        @pl.when(mine)
        def _():
            local(rxs.at[0], rbuf.at[0], lr.at[0]).wait()
            dha[ds] += rbuf[0]

        @pl.when(last)
        def _():
            local(rxb.at[0], rbuf.at[1], lr.at[1]).wait()
            dha[ds] += rbuf[1]
            local(dha.at[ds], dho.at[b], eo.at[ds]).start()

        @pl.when(jnp.logical_and(mine, r == 2))
        def _():
            local(dha.at[ds], txb.at[b], eo.at[ds]).start()

        @pl.when(jnp.logical_and(comp == 1, lax.rem(r, 2) == 1))
        def _():
            to_sib(r, b, ds).start()

        @pl.when(comp == 0)
        def _():
            local(dha.at[ds], part.at[i], eo.at[ds]).start()

        @pl.when(v == v_c - 1)
        def _():
            to_peer(0).start()

        @pl.when(v == v_e - 1)
        def _():
            to_peer(1).start()

    per = n_own // n_micro
    top = lax.broadcasted_iota(I32, (8, BT), 0) == 0
    for k in range(n_micro):
        tot = lse[blk(0, k * per)] - math.log2(tokens)
        for b in range(k * per + 1, (k + 1) * per):
            tot = tot + (lse[blk(0, b)] - math.log2(tokens))
        val = (jnp.where(top, tot, 0.0) - tla[k]) * (LN2 * inv)
        acc = val[:, :128]
        for c in range(128, BT, 128):
            acc = acc + val[:, c:c + 128]
        lmsg[k] = acc

    def send_loss(d):
        return remote(lmsg, lrx.at[d - 1], sl.at[d - 1], rl.at[d - 1], lax.rem(at.me + d, n))

    for d in range(1, n):
        send_loss(d).start()
    own_dw = local(dwa.at[pl.ds(0, 2)], dwo, lw.at[0])
    own_dw.start()
    finish(jnp.int32(n_visits - 2))
    finish(jnp.int32(n_visits - 1))
    for d in range(1, n):
        send_loss(d).wait()
    tot = lmsg[...]
    for d in range(n - 1):
        tot = tot + lrx[d]
    loss[...] = tot
    for k in range(2):
        to_peer(k).wait()
    for b in range(n_own):
        to_par(b).wait_send()
    own_dw.wait()


def solution(mesh):
    n = mesh.shape['fsdp']

    def local_head(hidden, targets, w_loc):
        n_micro, tok_dev, dim = hidden.shape
        vb = w_loc.shape[0]
        tokens = tok_dev * n
        rows = vb // 2
        n_own = n_micro * tok_dev // BT
        n_blk = 4 * n_own

        def out(shape, dtype=F32):
            return jax.ShapeDtypeStruct(shape, dtype)

        z, lse, hbuf, wpeer, tall = pl.pallas_call(
            functools.partial(fwd_kernel, n, tokens),
            out_shape=(out((4, n_blk, rows, BT)), out((n_blk, 1, BT)), out((n_blk, BT, dim), BF16), out((2, rows, dim), BF16),
                       out((n_blk, 1, BT), I32)),
            in_specs=[ANY, ANY, VM],
            out_specs=(ANY, VM, ANY, ANY, ANY),
            scratch_shapes=[
                pltpu.VMEM((4, rows, dim), BF16), pltpu.VMEM((n_blk, BT, dim), BF16), pltpu.VMEM((3, rows, BT), F32),
                pltpu.VMEM((n_blk, 8, BT), F32), pltpu.VMEM((n_blk, 8, BT), F32), pltpu.VMEM((2, n_blk, BT), F32),
                pltpu.VMEM((3, 2, n_blk, BT), F32),
                DMA((n_blk,)), DMA((2,)), DMA((2,)), DMA((2,)), DMA((n_own,)), DMA((n_own,)), DMA((n_own,)),
                DMA((3,)), DMA((3,)), DMA, DMA((n_blk,)), DMA((2,)), DMA((3,)), DMA((3,)), DMA((3,))],
            compiler_params=pltpu.CompilerParams(vmem_limit_bytes=VMEM_LIMIT, collective_id=0, has_side_effects=True),
            name='fwd',
        )(hidden.reshape(n_own, BT, dim), w_loc, targets.reshape(n_own, 1, BT))

        blk_shape = (dim, BT)
        dwo, rxw, dho, loss, *_ = pl.pallas_call(
            functools.partial(bwd_kernel, n, tokens, n_micro),
            out_shape=(out((2, rows, dim)), out((2, rows, dim)), out((n_own, *blk_shape)), out((n_micro, 8, 128)),
                       out((n_blk, *blk_shape)), out((2 * n_own, *blk_shape)), out((n_own, *blk_shape)), out((n_own, *blk_shape)),
                       out(blk_shape)),
            in_specs=[ANY, ANY, ANY, VM, VM, ANY],
            out_specs=(ANY, ANY, ANY, VM, ANY, ANY, ANY, ANY, ANY),
            scratch_shapes=[
                pltpu.VMEM((2, rows, dim), BF16), pltpu.VMEM((4, dim, up(rows, 256)), BF16), pltpu.VMEM((2, BT, dim), BF16),
                pltpu.VMEM((2, rows, BT), F32), pltpu.VMEM((4, rows, dim), F32), pltpu.VMEM((3, *blk_shape), F32),
                pltpu.VMEM((2, *blk_shape), F32), pltpu.VMEM((n_micro, 8, BT), F32), pltpu.VMEM((n_micro, 8, 128), F32),
                pltpu.VMEM((n - 1, n_micro, 8, 128), F32),
                DMA((2,)), DMA((2,)), DMA((2,)), DMA((3,)), DMA((2,)), DMA((3,)), DMA((3,)), DMA((2 * n_own,)),
                DMA((n_own,)), DMA((n_own,)), DMA((2,)), DMA((2,)), DMA((n - 1,)), DMA((n - 1,))],
            compiler_params=pltpu.CompilerParams(vmem_limit_bytes=VMEM_LIMIT, collective_id=1, has_side_effects=True),
            name='bwd',
        )(w_loc, wpeer, hbuf, tall, lse, z)

        d_w = (dwo + rxw).reshape(vb, dim)
        d_h = dho.transpose(0, 2, 1).reshape(n_micro, tok_dev, dim)
        return jnp.sum(loss, axis=(1, 2)), d_h, d_w

    return jax.shard_map(local_head, mesh=mesh,
                         in_specs=(P(None, ('dp', 'fsdp'), None), P(None, ('dp', 'fsdp')), P('fsdp', None)),
                         out_specs=(P('dp'), P(None, ('dp', 'fsdp'), None), P(('dp', 'fsdp'), None)),
                         check_vma=False)
```

```python
import functools
import math

import jax
import jax.numpy as jnp
from jax import lax
from jax.experimental import pallas as pl
from jax.experimental.pallas import tpu as pltpu
from jax.sharding import PartitionSpec as P

F32, BF16, I32 = jnp.float32, jnp.bfloat16, jnp.int32
LOG2E = 1.4426950408889634
LN2 = 0.6931471805599453
BT = 1024
RC = 256
N_PART = 4
VMEM_LIMIT = 61 << 20
ANY = pl.BlockSpec(memory_space=pl.ANY)
VM = pl.BlockSpec(memory_space=pltpu.VMEM)
DMA = pltpu.SemaphoreType.DMA
local = pltpu.make_async_copy


def remote(src, dst, send_sem, recv_sem, to):
    return pltpu.make_async_remote_copy(src_ref=src, dst_ref=dst, send_sem=send_sem, recv_sem=recv_sem,
                                        device_id={'fsdp': to}, device_id_type=pl.DeviceIdType.MESH)


def chunks(rows):
    return [(r0, min(RC, rows - r0)) for r0 in range(0, rows, RC)]


def up(a, b):
    return -(-a // b) * b


def pick(x, segments):
    out = segments[0][1]
    for lo, vals in segments[1:]:
        out = tuple(jnp.where(x >= lo, a, b) for a, b in zip(vals, out))
    return out


class Place:
    def __init__(self, n):
        self.me = lax.axis_index('fsdp')
        self.chip, self.core = self.me // 2, lax.rem(self.me, 2)
        self.odd = lax.rem(self.chip, 2)
        self.sib = self.me + 1 - 2 * self.core
        self.par = self.me + 2 - 4 * self.odd
        self.diag = self.sib + 2 - 4 * self.odd
        self.peer = lax.rem(self.chip + 2 * self.odd - 1 + n // 2, n // 2) * 2 + self.core

    def share(self, r):
        a, b = lax.rem(r, 2), r // 2
        return 2 * (self.odd + b - 2 * self.odd * b) + self.core + a - 2 * self.core * a


def barrier_with(others):
    sem = pltpu.get_barrier_semaphore()
    for d in others:
        pl.semaphore_signal(sem, inc=1, device_id={'fsdp': d}, device_id_type=pl.DeviceIdType.MESH)
    pl.semaphore_wait(sem, len(others))


def fwd_unit(w_ref, h_ref, z_ref, m_ref, s_ref):
    rows = w_ref.shape[0]
    h = h_ref[...]
    m, s = m_ref[...], s_ref[...]
    for r0, rc in chunks(rows):
        z = lax.dot_general(w_ref[r0:r0 + rc, :], h, (((1,), (1,)), ((), ())), preferred_element_type=F32) * LOG2E
        z_ref[r0:r0 + rc, :] = z
        z = z.reshape(rc // 8, 8, BT)
        mn = jnp.maximum(m, jnp.max(z, axis=0))
        s = s * jnp.exp2(m - mn) + jnp.sum(jnp.exp2(z - mn[None]), axis=0)
        m = mn
    m_ref[...], s_ref[...] = m, s


def bwd_unit(z_ref, lse, tgt, inv, w_ref, h_ref, dw_ref, dh_ref, tl_ref):
    rows = z_ref.shape[0]
    h = h_ref[...]
    tj = tgt - lax.broadcasted_iota(I32, (8, BT), 0)
    tl = jnp.zeros((8, BT), F32)
    acc = None
    for r0, rc in chunks(rows):
        z = z_ref[r0:r0 + rc, :].reshape(rc // 8, 8, BT)
        p = jnp.exp2(z - lse[None])
        hit = lax.broadcasted_iota(I32, (rc // 8, 8, BT), 0) * 8 + r0 == tj[None]
        dz = jnp.where(hit, p - inv, p).reshape(rc, BT)
        for k in range(rc // 8):
            tl = jnp.where(hit[k], z[k], tl)
        rk, rm = up(rc, 256), up(rc, 16)
        if rk > rc:
            dz = jnp.concatenate([dz, jnp.zeros((rk - rc, BT), F32)], axis=0)
        dz = dz.astype(BF16)
        d = jnp.dot(dz[:rm], h, preferred_element_type=F32)
        dw_ref[r0:r0 + rc, :] += d[:rc]
        d = lax.dot_general(dz, w_ref[r0:r0 + rk, :], (((0,), (0,)), ((), ())), preferred_element_type=F32)
        acc = d if acc is None else acc + d
    dh_ref[...] += acc
    tl_ref[...] += tl


def fwd_kernel(n, tokens, hid, w, tg, z, lse, hbuf, wpeer, tall, wv, hv, zv, m, s, st, strx,
               rh, lw, rw, sw, shs, shp, sf, stt, rt, lt, oh, ow, oz, ss, rs):
    at = Place(n)
    n_own = hid.shape[0]
    rows = wv.shape[1]
    quad = (at.me, at.sib, at.par, at.diag)

    def blk(r, b):
        return n_own * at.share(r) + b

    half_src = [w.at[pl.ds(k * rows, rows)] for k in range(2)]
    for k in range(2):
        local(half_src[k], wv.at[k], lw.at[k]).start()
    for b in range(n_own):
        local(hid.at[b], hv.at[blk(0, b)], rh.at[b]).start()
    own_t = tall.at[pl.ds(n_own * at.share(0), n_own)]
    local(tg, own_t, lt).start()

    barrier_with([at.sib, at.par, at.diag, at.peer])

    def send_sib(b):
        return remote(hid.at[b], hv.at[blk(0, b)], shs.at[b], rh.at[n_own + b], at.sib)

    def send_par(b):
        return remote(hid.at[b], hv.at[blk(0, b)], shp.at[b], rh.at[2 * n_own + b], at.par)

    def forward(b):
        return remote(hv.at[blk(2, b)], hv.at[blk(2, b)], sf.at[b], rh.at[3 * n_own + b], at.sib)

    def send_w(k):
        return remote(half_src[k], wv.at[2 + k], sw.at[k], rw.at[k], at.peer)

    def send_t(r):
        return remote(tg, own_t, stt.at[r - 1], rt.at[r - 1], quad[r])

    def send_st(r):
        return remote(st, strx.at[r - 1], ss.at[r - 1], rs.at[r - 1], quad[r])

    for k in range(n_own):
        send_sib(k).start()
        send_par(k).start()
        if k < 2:
            send_w(k).start()
    for r in range(1, 4):
        send_t(r).start()

    m[...] = jnp.full_like(m, -jnp.inf)
    s[...] = jnp.zeros_like(s)

    s2 = 4 * n_own
    s3 = s2 + 4
    s4 = s3 + 2 * n_own
    s5 = s4 + 4 * (n_own - 2)
    s6 = s5 + 2 * n_own
    s7 = s6 + 4
    first2, first3 = s3, s5

    def order(u):
        def near(q):
            return lax.rem(q, 2), q // (2 * n_own), lax.rem(q // 2, n_own)

        def far(q, b0):
            return lax.rem(q, 2), 2 + lax.rem(q // 2, 2), b0 + q // 4

        def wide(q, h):
            return jnp.full_like(q, h), q // n_own, lax.rem(q, n_own)

        h7, r7, b7 = far(u - s7, 0)
        return pick(u, [(0, near(u)), (s2, far(u - s2, 0)), (s3, wide(u - s3, 2)), (s4, far(u - s4, 1)),
                        (s5, wide(u - s5, 3)), (s6, far(u - s6, n_own - 1)), (s7, (h7 + 2, r7, b7))])

    n_units = 4 * 4 * n_own

    parts = [(q, min(rows, q + up(-(-rows // N_PART), 8))) for q in range(0, rows, up(-(-rows // N_PART), 8))]

    def store_z(h, i, slot):
        for lo, hi in parts:
            local(zv.at[slot, pl.ds(lo, hi - lo)], z.at[h, i, pl.ds(lo, hi - lo)], oz.at[slot]).start()

    def wait_z(slot):
        local(zv.at[slot], z.at[0, 0], oz.at[slot]).wait()

    def body(u, unit):
        h, r, b, i = unit
        slot = lax.rem(u, 3)

        @pl.when(u < 2)
        def _():
            local(half_src[0], wv.at[u], lw.at[u]).wait()

        @pl.when(jnp.logical_or(u == first2, u == first3))
        def _():
            remote(half_src[0], wv.at[h], sw.at[0], rw.at[h - 2], at.peer).wait_recv()
            local(wv.at[h], wpeer.at[h - 2], ow.at[h - 2]).start()

        @pl.when(h == 0)
        def _():
            @pl.when(r == 0)
            def _():
                local(hid.at[0], hv.at[i], rh.at[b]).wait()

            @pl.when(r > 0)
            def _():
                remote(hid.at[0], hv.at[i], shs.at[0], rh.at[n_own * r + b], at.sib).wait_recv()

            local(hv.at[i], hbuf.at[i], oh.at[i]).start()

            @pl.when(r == 2)
            def _():
                forward(b).start()

        @pl.when(u >= 3)
        def _():
            wait_z(slot)

        fwd_unit(wv.at[h], hv.at[i], zv.at[slot], m.at[i], s.at[i])
        nh, nr, nb = order(u + 1)
        ni = blk(nr, nb)
        store_z(h, i, slot)
        return nh, nr, nb, ni

    start = order(jnp.int32(0))
    lax.fori_loop(0, n_units, body, (*start, blk(start[1], start[2])))

    mm = m[...]
    m1 = jnp.max(mm, axis=1, keepdims=True)
    st[0] = m1[:, 0, :]
    st[1] = jnp.sum(s[...] * jnp.exp2(mm - m1), axis=1)
    for r in range(1, 4):
        send_st(r).start()
    for r in range(1, 4):
        send_t(r).wait()
        send_st(r).wait()
    mx = st[0]
    for r in range(3):
        mx = jnp.maximum(mx, strx[r, 0])
    tot = st[1] * jnp.exp2(st[0] - mx)
    for r in range(3):
        tot = tot + strx[r, 1] * jnp.exp2(strx[r, 0] - mx)
    lse[...] = (mx + jnp.log(tot) * LOG2E + math.log2(tokens)).reshape(lse.shape)

    local(tg, own_t, lt).wait()
    for k in range(n_own):
        send_sib(k).wait_send()
        send_par(k).wait_send()
        forward(k).wait_send()
    for k in range(2):
        send_w(k).wait_send()
        local(wv.at[2 + k], wpeer.at[k], ow.at[k]).wait()
    for k in range(4 * n_own):
        local(hv.at[k], hbuf.at[k], oh.at[k]).wait()
    for k in range(3):
        wait_z(k)


def bwd_kernel(n, tokens, n_micro, w, wpeer, hbuf, tall, lse, z, dwo, dho, loss, rxw, part, rxs, txb, rxb, zblk,
               wv, hv, zv, dwa, dha, rbuf, tla, lmsg, lrx,
               lw, lz, lh, li, lr, eo, es, rss, sb, rb, swr, rwr, sl, rl):
    at = Place(n)
    n_own = dho.shape[0]
    rows, cols = zv.shape[1], wv.shape[1]
    dim = wv.shape[2]
    inv = 1.0 / tokens

    sem = pltpu.get_barrier_semaphore()
    for d in range(1, n):
        pl.semaphore_signal(sem, inc=1, device_id={'fsdp': lax.rem(at.me + d, n)}, device_id_type=pl.DeviceIdType.MESH)

    def blk(r, b):
        return n_own * at.share(r) + b

    far = 2 * (n_own - 1)
    v_b, v_c = 2, 2 + far + 2 * n_own
    v_d = v_c + far - 2
    v_e = v_d + 2 + 2 * n_own
    v_f = v_e + 2
    u_b = 8
    u_c = u_b + far + 2 * n_own
    u_d = u_c + 3 * (far - 2)
    u_e = u_d + 2 + 2 * n_own
    u_f = u_e + 4
    n_units = u_f + 4 * n_own
    n_visits = v_f + 2 * n_own

    def order(u):
        def far_pair(q, b0):
            return 3 - lax.rem(q, 2), b0 + q // 2

        def near_pair(q):
            return 1 - lax.rem(q, 2), q // 2

        one = jnp.ones_like(u)
        zero = one - 1

        def run(q, count, h0, pair, v0, fresh):
            k, wv_ = lax.rem(q, count), lax.div(q, jnp.int32(count))
            return (lax.rem(k + h0, 4), *pair(wv_), (k == 0).astype(I32), (k == count - 1).astype(I32), v0 + wv_, fresh, one)

        def sweep(q, h, pair, v0, fresh):
            return (h * one, *pair, one, one, v0 + q, fresh, zero)

        qb, qd = u - u_b, u - u_d
        return pick(u, [
            (0, run(u, 4, 0, lambda q: far_pair(q, 0), 0, one)),
            (u_b, sweep(qb, 2, far_pair(qb, 1), v_b, one)),
            (u_b + far, sweep(qb, 2, near_pair(qb - far), v_b, one)),
            (u_c, run(u - u_c, 3, 3, lambda q: far_pair(q, 1), v_c, zero)),
            (u_d, sweep(qd, 3, far_pair(qd, n_own - 1), v_d, zero)),
            (u_d + 2, sweep(qd, 3, near_pair(qd - 2), v_d, zero)),
            (u_e, run(u - u_e, 2, 0, lambda q: far_pair(q, n_own - 1), v_e, zero)),
            (u_f, run(u - u_f, 2, 0, near_pair, v_f, zero)),
        ])

    def load_z(h, i, slot):
        return local(z.at[h, i], zv.at[slot], lz.at[slot])

    def load_h(i, slot):
        return local(hbuf.at[i], hv.at[slot], lh.at[slot])

    def to_sib(r, b, slot):
        return remote(dha.at[slot], rxs.at[n_own * (1 - r // 2) + b], es.at[slot], rss.at[n_own * (1 - r // 2) + b], at.sib)

    def from_sib(r, b):
        return remote(dha.at[0], rxs.at[n_own * (1 - r // 2) + b], es.at[0], rss.at[n_own * (1 - r // 2) + b], at.sib)

    def to_par(b):
        return remote(txb.at[b], rxb.at[b], sb.at[b], rb.at[b], at.par)

    def to_peer(k):
        return remote(dwa.at[2 + k], rxw.at[k], swr.at[k], rwr.at[k], at.peer)

    def load_rx(k):
        return local(rxw.at[k], zv.at[0, :, pl.ds(k * dim, dim)], lr.at[2 + k])

    halves = [w.at[pl.ds(0, rows)], w.at[pl.ds(rows, rows)], wpeer.at[0], wpeer.at[1]]

    def load_w(k):
        return local(halves[k], wv.at[k, pl.ds(0, rows)], lw.at[k])

    load_w(0).start()
    load_z(0, blk(3, 0), 0).start()
    load_h(blk(3, 0), 0).start()
    for k in range(1, 4):
        load_w(k).start()
    rbuf[0] = jnp.zeros(rbuf.shape[1:], F32)
    local(rbuf.at[0], zblk, lr.at[0]).start()
    if cols > rows:
        for k in range(4):
            wv[k, rows:] = jnp.zeros((cols - rows, dim), BF16)
    dha[0] = jnp.zeros(dha.shape[1:], F32)
    dwa[...] = jnp.zeros_like(dwa)
    tla[...] = jnp.zeros_like(tla)
    local(rbuf.at[0], zblk, lr.at[0]).wait()
    pl.semaphore_wait(sem, n - 1)

    def finish(r, b, comp, slot):
        sent = jnp.logical_and(comp == 1, lax.rem(r, 2) == 1)

        @pl.when(sent)
        def _():
            to_sib(r, b, slot).wait_send()

        @pl.when(jnp.logical_not(sent))
        def _():
            local(dha.at[slot], part.at[0], eo.at[slot]).wait()

        @pl.when(jnp.logical_and(comp == 1, r == 2))
        def _():
            to_par(b).start()

    def body(u, carry):
        unit, i, nxt, i_n, p1, p2 = carry
        h, r, b, opens, closes, v, _, comp = unit
        h_n, fresh_n = nxt[0], nxt[6]
        slot, hs, ds, ds_n = lax.rem(u, 2), lax.rem(v, 2), lax.rem(v, 3), lax.rem(v + 1, 3)
        more = u + 1 < n_units
        odd = lax.rem(r, 2) == 1
        ends = jnp.logical_and(closes == 1, comp == 1)
        mine = jnp.logical_and(ends, jnp.logical_not(odd))
        last = jnp.logical_and(mine, r == 0)

        @pl.when(u < 4)
        def _():
            local(halves[0], wv.at[h, pl.ds(0, rows)], lw.at[h]).wait()

        load_z(h, i, slot).wait()

        @pl.when(more)
        def _():
            load_z(h_n, i_n, 1 - slot).start()

        @pl.when(opens == 1)
        def _():
            @pl.when(v >= 2)
            def _():
                finish(*p2, ds_n)

            load_h(i, hs).wait()

            @pl.when(v > 0)
            def _():
                local(zblk, dha.at[ds], li.at[ds]).wait()

        @pl.when(closes == 1)
        def _():
            @pl.when(more)
            def _():
                load_h(i_n, 1 - hs).start()

                @pl.when(fresh_n == 1)
                def _():
                    local(zblk, dha.at[ds_n], li.at[ds_n]).start()

                @pl.when(fresh_n == 0)
                def _():
                    local(part.at[i_n], dha.at[ds_n], li.at[ds_n]).start()

            @pl.when(jnp.logical_not(more))
            def _():
                for k in range(2):
                    to_peer(k).wait_recv()
                    load_rx(k).start()

            @pl.when(mine)
            def _():
                from_sib(r, b).wait_recv()
                local(rxs.at[n_own * (1 - r // 2) + b], rbuf.at[0], lr.at[0]).start()

            @pl.when(last)
            def _():
                to_par(b).wait_recv()
                local(rxb.at[b], rbuf.at[1], lr.at[1]).start()

        base = jnp.where(h < 2, at.me, at.peer) * (2 * rows) + lax.rem(h, 2) * rows
        bwd_unit(zv.at[slot], lse[i], tall[i] - base, inv, wv.at[h], hv.at[hs], dwa.at[h], dha.at[ds],
                 tla.at[b // (n_own // n_micro)])
        after = order(u + 2)
        i_after = blk(after[1], after[2])
        shift = closes == 1
        q2 = tuple(jnp.where(shift, x, y) for x, y in zip(p1, p2))
        q1 = tuple(jnp.where(shift, x, y) for x, y in zip((r, b, comp), p1))

        @pl.when(closes == 1)
        def _():
            @pl.when(mine)
            def _():
                local(rxs.at[0], rbuf.at[0], lr.at[0]).wait()

                @pl.when(r == 0)
                def _():
                    local(rxb.at[0], rbuf.at[1], lr.at[1]).wait()
                    dha[ds] += rbuf[0] + rbuf[1]
                    local(dha.at[ds], dho.at[b], eo.at[ds]).start()

                @pl.when(r == 2)
                def _():
                    dha[ds] += rbuf[0]
                    local(dha.at[ds], txb.at[b], eo.at[ds]).start()

            @pl.when(jnp.logical_and(ends, odd))
            def _():
                to_sib(r, b, ds).start()

            @pl.when(comp == 0)
            def _():
                local(dha.at[ds], part.at[i], eo.at[ds]).start()

                @pl.when(u == u_c - 1)
                def _():
                    to_peer(0).start()

                @pl.when(u == u_e - 1)
                def _():
                    to_peer(1).start()

        return nxt, i_n, after, i_after, q1, q2

    first, second = order(jnp.int32(0)), order(jnp.int32(1))
    none = (jnp.int32(0),) * 3
    _, _, _, _, p1, p2 = lax.fori_loop(
        0, n_units, body, (first, blk(first[1], first[2]), second, blk(second[1], second[2]), none, none))

    per = n_own // n_micro
    top = lax.broadcasted_iota(I32, (8, BT), 0) == 0
    for k in range(n_micro):
        tot = lse[blk(0, k * per)] - math.log2(tokens)
        for b in range(k * per + 1, (k + 1) * per):
            tot = tot + (lse[blk(0, b)] - math.log2(tokens))
        val = (jnp.where(top, tot, 0.0) - tla[k]) * (LN2 * inv)
        acc = val[:, :128]
        for c in range(128, BT, 128):
            acc = acc + val[:, c:c + 128]
        lmsg[k] = acc

    def send_loss(d):
        return remote(lmsg, lrx.at[d - 1], sl.at[d - 1], rl.at[d - 1], lax.rem(at.me + d, n))

    for d in range(1, n):
        send_loss(d).start()
    edges = [rows * q // 32 * 8 for q in range(4)] + [rows]
    pieces = list(zip(edges[:-1], edges[1:]))

    def out_dw(k):
        return local(dwa.at[k], dwo.at[k], lw.at[k])

    for k in range(2):
        load_rx(k).wait()
        for lo, hi in pieces:
            dwa[k, lo:hi] += zv[0, lo:hi, k * dim:(k + 1) * dim]
            local(dwa.at[k, pl.ds(lo, hi - lo)], dwo.at[k, pl.ds(lo, hi - lo)], lw.at[k]).start()
    finish(*p2, lax.rem(jnp.int32(n_visits - 2), 3))
    finish(*p1, lax.rem(jnp.int32(n_visits - 1), 3))
    for d in range(1, n):
        send_loss(d).wait()
    tot = lmsg[...]
    for d in range(n - 1):
        tot = tot + lrx[d]
    loss[...] = tot
    for k in range(2):
        to_peer(k).wait_send()
    for b in range(n_own):
        to_par(b).wait_send()
    for k in range(2):
        out_dw(k).wait()


def solution(mesh):
    n = mesh.shape['fsdp']

    def local_head(hidden, targets, w_loc):
        n_micro, tok_dev, dim = hidden.shape
        vb = w_loc.shape[0]
        tokens = tok_dev * n
        rows = vb // 2
        n_own = n_micro * tok_dev // BT
        n_blk = 4 * n_own

        def out(shape, dtype=F32):
            return jax.ShapeDtypeStruct(shape, dtype)

        z, lse, hbuf, wpeer, tall = pl.pallas_call(
            functools.partial(fwd_kernel, n, tokens),
            out_shape=(out((4, n_blk, rows, BT)), out((n_blk, 1, BT)), out((n_blk, BT, dim), BF16), out((2, rows, dim), BF16),
                       out((n_blk, 1, BT), I32)),
            in_specs=[ANY, ANY, VM],
            out_specs=(ANY, VM, ANY, ANY, ANY),
            scratch_shapes=[
                pltpu.VMEM((4, rows, dim), BF16), pltpu.VMEM((n_blk, BT, dim), BF16), pltpu.VMEM((3, rows, BT), F32),
                pltpu.VMEM((n_blk, 8, BT), F32), pltpu.VMEM((n_blk, 8, BT), F32), pltpu.VMEM((2, n_blk, BT), F32),
                pltpu.VMEM((3, 2, n_blk, BT), F32),
                DMA((n_blk,)), DMA((2,)), DMA((2,)), DMA((2,)), DMA((n_own,)), DMA((n_own,)), DMA((n_own,)),
                DMA((3,)), DMA((3,)), DMA, DMA((n_blk,)), DMA((2,)), DMA((3,)), DMA((3,)), DMA((3,))],
            compiler_params=pltpu.CompilerParams(vmem_limit_bytes=VMEM_LIMIT, collective_id=0, has_side_effects=True),
            name='fwd',
        )(hidden.reshape(n_own, BT, dim), w_loc, targets.reshape(n_own, 1, BT))

        blk_shape = (BT, dim)
        dwo, dho, loss, *_ = pl.pallas_call(
            functools.partial(bwd_kernel, n, tokens, n_micro),
            out_shape=(out((2, rows, dim)), out((n_own, *blk_shape)), out((n_micro, 8, 128)), out((2, rows, dim)),
                       out((n_blk, *blk_shape)), out((2 * n_own, *blk_shape)), out((n_own, *blk_shape)), out((n_own, *blk_shape)),
                       out(blk_shape)),
            in_specs=[ANY, ANY, ANY, VM, VM, ANY],
            out_specs=(ANY, ANY, VM, ANY, ANY, ANY, ANY, ANY, ANY),
            scratch_shapes=[
                pltpu.VMEM((4, up(rows, 256), dim), BF16), pltpu.VMEM((2, BT, dim), BF16),
                pltpu.VMEM((2, rows, BT), F32), pltpu.VMEM((4, rows, dim), F32), pltpu.VMEM((3, *blk_shape), F32),
                pltpu.VMEM((2, *blk_shape), F32), pltpu.VMEM((n_micro, 8, BT), F32),
                pltpu.VMEM((n_micro, 8, 128), F32), pltpu.VMEM((n - 1, n_micro, 8, 128), F32),
                DMA((4,)), DMA((2,)), DMA((2,)), DMA((3,)), DMA((4,)), DMA((3,)), DMA((3,)), DMA((2 * n_own,)),
                DMA((n_own,)), DMA((n_own,)), DMA((2,)), DMA((2,)), DMA((n - 1,)), DMA((n - 1,))],
            compiler_params=pltpu.CompilerParams(vmem_limit_bytes=VMEM_LIMIT, collective_id=1, has_side_effects=True),
            name='bwd',
        )(w_loc, wpeer, hbuf, tall, lse, z)

        d_w = dwo.reshape(vb, dim)
        d_h = dho.reshape(n_micro, tok_dev, dim)
        return jnp.sum(loss, axis=(1, 2)), d_h, d_w

    return jax.shard_map(local_head, mesh=mesh,
                         in_specs=(P(None, ('dp', 'fsdp'), None), P(None, ('dp', 'fsdp')), P('fsdp', None)),
                         out_specs=(P('dp'), P(None, ('dp', 'fsdp'), None), P(('dp', 'fsdp'), None)),
                         check_vma=False)
```
